32 devices in a mesh: parts: 2 (over x), dp: 16 (over z, y, core).
Axes of the slice: x: 2, y: 2, z: 4, core: 2. Of those that a mesh axis runs over, the one named last changes fastest.
Arguments:
- train_grads: bfloat16 [16384, 4096], P(('parts', 'dp')), parts along dimension 0, may hold values from -160 to 160
- query_grads: bfloat16 [768, 4096], P(('parts', 'dp')), parts along dimension 0, may hold values from -0.29882812 to 0.29882812
- in_basis: bfloat16 [4, 32, 32], replicated, may hold values from -1 to 1
- out_basis: bfloat16 [4, 32, 32], replicated, may hold values from -1 to 1
- damping: float32 [2], replicated, may hold values from 0.05 to 1
- layer_group: int32 [4], replicated, may hold values from 0 to 1, as said below
Outputs:
- scores: float32 [16384, 384], P(('parts', 'dp')), parts along dimension 0
The draws below stay inside these ranges and needn't reach their ends.
There are 2 independent parts, one for each index of `parts`. The reference program is written for one: setup_inputs(seed, part) draws one part's arguments, and reference() takes and returns one part's arrays. A program takes and returns all parts, laid end to end along the dimension named above; an argument that names none is the same for every part. Nothing has to cross between parts.
Inputs may be any that keep to these rules, and one draw needn't show every extreme that they name: `layer_group`: every group holds at least one layer.
All inputs are finite; a program needn't handle non-finite values.
Results may differ from the reference program's by a relative error of at most 0.0065.
Values may be sent and summed in bfloat16 or wider, within the bound.
No kernel may reach another device: no remote copies, remote signals or barrier semaphores. Data moves between devices by JAX's collectives and lax.ppermute only.
A program may use at most 128 MiB of HBM per device.

```python
import math
import jax
import jax.numpy as jnp
from jax import lax

R = 32
L = 4
NG = 2
TRAIN = 8192
Q = 384


def draw_train_grads(key, part):
    first = jax.random.fold_in(key, 0)
    positions = jnp.arange(TRAIN, dtype=jnp.float32)
    rising = 1.0 + 2.0 * positions / max(TRAIN - 1, 1)
    values = jnp.clip(jax.random.normal(first, (TRAIN, L * R * R), jnp.float32), -6.0, 6.0) * rising[:, None]
    return jnp.clip(values, -160.0, 160.0).astype(jnp.bfloat16)


def draw_layer_group(key, part):
    first, second = jax.random.split(jax.random.fold_in(key, 17))
    chosen = jax.random.randint(first, (L,), 0, NG, dtype=jnp.int32)
    order = jax.random.permutation(second, L)
    chosen = chosen.at[order[:NG]].set(jnp.arange(NG, dtype=jnp.int32))
    return chosen.astype(jnp.int32)


def block_levels(key, extent, pieces, least, high):
    factor_of = 1.0
    for dim, shards_of in pieces:
        draws = jax.random.uniform(jax.random.fold_in(jax.random.fold_in(key, 6), dim), (shards_of,), jnp.float32, least / len(pieces), high / len(pieces))
        factor_of = factor_of * jnp.repeat(jnp.exp(draws), extent[dim] // shards_of).reshape((-1,) + (1,) * (len(extent) - 1 - dim))
    return factor_of


def bell_draw(own_key, extent, deviation, most, shards=(), held_as=jnp.bfloat16):
    values = jax.random.normal(own_key, extent, jnp.float32) * deviation
    if len(shards) > 0:
        values = block_levels(own_key, extent, shards, -0.22, 0.18) * values
    return jnp.clip(values, min=-most, max=most).astype(held_as)


def setup_inputs(seed: int = 0, part: int = 0) -> dict:
    seeds = jax.random.split(jax.random.key(seed), 7)
    part_splits = jax.random.split(jax.random.fold_in(seeds[6], part), 7)
    train_grads = draw_train_grads(jax.random.fold_in(jax.random.fold_in(seeds[6], part), 71), part)
    query_grads = bell_draw(part_splits[1], (Q, L * R * R), 0.05, 0.29882812, ((0, 16),))
    in_basis = bell_draw(seeds[2], (L, R, R), R ** -0.5, 1.0)
    out_basis = bell_draw(seeds[3], (L, R, R), R ** -0.5, 1.0)
    damping = jnp.clip(jnp.exp(jax.random.uniform(seeds[4], (NG,), jnp.float32, math.log(0.05), math.log(1.0))), 0.05, 1.0)
    layer_group = draw_layer_group(jax.random.fold_in(seeds[6], 71), part)
    return {"train_grads": train_grads, "query_grads": query_grads, "in_basis": in_basis, "out_basis": out_basis, "damping": damping, "layer_group": layer_group}


def rotate(grads, in_basis, out_basis):
    rows = grads.shape[0]
    shaped = grads.astype(jnp.float32).reshape(rows, L, R, R)
    inner = jnp.einsum('tlij,ljb->tlib', shaped, in_basis.astype(jnp.float32), precision=lax.Precision.HIGHEST)
    inner = inner.astype(jnp.bfloat16).astype(jnp.float32)
    outer = jnp.einsum('tlib,lia->tlab', inner, out_basis.astype(jnp.float32), precision=lax.Precision.HIGHEST)
    return outer.reshape(rows, L * R * R)


def reference(train_grads, query_grads, in_basis, out_basis, damping, layer_group):
    rotated = rotate(train_grads, in_basis, out_basis)
    corrected = (jnp.sum(rotated * rotated, axis=0) / TRAIN).reshape(L, R * R)
    pick = (layer_group[:, None] == jnp.arange(NG, dtype=jnp.int32)[None, :]).astype(jnp.float32)
    per_layer = jnp.sum(pick * damping[None, :], axis=1)
    denominator = (corrected + per_layer[:, None] * jnp.mean(corrected, axis=1, keepdims=True)).reshape(-1)
    train_rounded = rotated.astype(jnp.bfloat16)
    preconditioned = (rotate(query_grads, in_basis, out_basis) / denominator).astype(jnp.bfloat16)
    return jnp.dot(train_rounded.astype(jnp.float32), preconditioned.astype(jnp.float32).T, precision=lax.Precision.HIGHEST)
```

```python
import functools

import jax
import jax.numpy as jnp
from jax import lax
from jax.experimental import pallas as pl
from jax.experimental.pallas import tpu as pltpu
from jax.sharding import PartitionSpec as P


LANES = 128
MIB = 1024 * 1024
VMEM = pl.BlockSpec(memory_space=pltpu.VMEM)
SMEM = pl.BlockSpec(memory_space=pltpu.SMEM)
HBM = pl.BlockSpec(memory_space=pltpu.HBM)


def stage_matrices(in_ref, out_ref, width):
    layers = in_ref.shape[0]
    group = 2 * LANES // width
    half = LANES // group
    cols, wide = 2 * LANES, half * width

    def iota(shape, dim):
        return lax.broadcasted_iota(jnp.int32, shape, dim)

    spread = iota((width, cols), 1) // group == iota((width, cols), 0)
    repeat = iota((width, wide), 1) % width == iota((width, wide), 0)
    flat_in = in_ref[...].reshape(layers * width, width)
    flat_out = out_ref[...].reshape(layers * width, width)
    wide_in = jnp.dot(flat_in, spread.astype(jnp.bfloat16), preferred_element_type=jnp.float32)
    wide_out = jnp.dot(flat_out, repeat.astype(jnp.bfloat16), preferred_element_type=jnp.float32)
    which = iota((width, cols), 1) % group
    keep = iota((LANES, wide), 0) // group == iota((LANES, wide), 1) // width
    firsts, seconds = [], []
    for l in range(layers):
        rows = wide_in[l * width : (l + 1) * width]
        first = [jnp.where(which == i, rows, 0.0) for i in range(group)]
        firsts.append(jnp.concatenate(first, axis=0).astype(jnp.bfloat16))
        second = []
        for k in range(width // group):
            at = l * width + k * group
            tiled = jnp.concatenate([wide_out[at : at + group]] * half, axis=0)
            second.append(jnp.where(keep, tiled, 0.0))
        seconds.append(jnp.concatenate(second, axis=0).astype(jnp.bfloat16))
    return firsts, seconds


def rotate_layer(x_ref, base, first, second, width):
    cols = 2 * LANES
    inner = []
    for k in range(width * width // cols):
        at = base + k * cols
        inner.append(
            jnp.dot(x_ref[:, at : at + cols], first, preferred_element_type=jnp.float32).astype(
                jnp.bfloat16
            )
        )
    for h in range(2):
        lhs = jnp.concatenate([x[:, h * LANES : (h + 1) * LANES] for x in inner], axis=1)
        yield jnp.dot(lhs, second, preferred_element_type=jnp.float32)


def prepare_kernel(
    layers,
    width,
    q_hbm,
    in_hbm,
    out_hbm,
    x_hbm,
    rot_ref,
    first_ref,
    second_ref,
    held_ref,
    q_ref,
    in_ref,
    out_ref,
    sems,
):
    ends = ((in_hbm, in_ref), (out_hbm, out_ref), (q_hbm, q_ref), (x_hbm, held_ref))
    copies = [pltpu.make_async_copy(a, b, sems.at[i]) for i, (a, b) in enumerate(ends)]
    for copy in copies:
        copy.start()
    for copy in copies[:3]:
        copy.wait()
    firsts, seconds = stage_matrices(in_ref, out_ref, width)
    rows = q_ref.shape[0]
    cols, block = 2 * LANES, width * width
    tiles = block // cols
    inners = []
    for l in range(layers):
        stack = [
            q_ref[:, l * block + k * cols : l * block + (k + 1) * cols].astype(jnp.float32)
            for k in range(tiles)
        ]
        stack = jnp.concatenate(stack, axis=0).astype(jnp.bfloat16)
        inners.append(jnp.dot(stack, firsts[l], preferred_element_type=jnp.float32))
    for l in range(layers):
        halves = [
            jnp.concatenate(
                [
                    inners[l][k * rows : (k + 1) * rows, h * LANES : (h + 1) * LANES]
                    for k in range(tiles)
                ],
                axis=1,
            )
            for h in range(2)
        ]
        lhs = jnp.concatenate(halves, axis=0).astype(jnp.bfloat16)
        rotated = jnp.dot(lhs, seconds[l], preferred_element_type=jnp.float32).astype(jnp.bfloat16)
        at = l * block
        for h in range(2):
            rot_ref[:, at : at + block // 2] = rotated[h * rows : (h + 1) * rows]
            at += block // 2
    for l in range(layers):
        first_ref[l] = firsts[l]
        second_ref[l] = seconds[l]
    copies[3].wait()


def train_kernel(layers, width, x_ref, first_ref, second_ref, rot_ref, sums_ref):
    block = width * width
    for l in range(layers):
        at = l * block
        for rotated in rotate_layer(x_ref, l * block, first_ref[l], second_ref[l], width):
            rot_ref[:, at : at + block // 2] = rotated.astype(jnp.bfloat16)
            sums_ref[:, at : at + block // 2] = jnp.sum(rotated * rotated, axis=0, keepdims=True)
            at += block // 2


def score_kernel(
    layers, steps, rows, train_rows, group_ref, damp_ref, sums_ref, rot_ref, *refs
):
    count = len(steps)
    chips = lax.axis_size("dp") // 2
    me = lax.axis_index("dp")
    chip, mine = me // 2, me % 2
    spot = jnp.where(chip % 2 == 0, chip // 2, chips - 1 - chip // 2)
    pieces, score_ref, scaled = refs[:count], refs[-2], refs[-1]
    block = sums_ref.shape[1] // layers
    spots = []
    for step, twin in steps:
        at = (spot - step + chips) % chips
        first = jnp.where(at < chips // 2, 2 * at, 2 * (chips - 1 - at) + 1) * 2
        spots.append(pl.multiple_of((first + (mine ^ twin)) * rows, 8))

    def fill(l, lanes, slot):
        corrected = sums_ref[:, lanes] / train_rows
        damp = damp_ref[group_ref[l]]
        inverse = 1.0 / (corrected + damp * jnp.mean(corrected, axis=1, keepdims=True))
        for where, piece in zip(spots, pieces):
            scaled[slot, pl.ds(where, rows), :] = piece[:, lanes].astype(jnp.float32) * inverse

    def dot(lanes, right):
        return lax.dot_general(
            rot_ref[:, lanes],
            right.astype(jnp.bfloat16),
            (((1,), (1,)), ((), ())),
            preferred_element_type=jnp.float32,
        )

    if scaled.shape[0] == layers:
        total = None
        for l in range(layers):
            fill(l, slice(l * block, (l + 1) * block), l)
        for l in range(layers):
            product = dot(slice(l * block, (l + 1) * block), scaled[l])
            total = product if total is None else total + product
        score_ref[...] = total
        return

    queries = score_ref.shape[1]
    chunk = next(n for n in (512, 384, 256, 128, queries) if queries % n == 0)
    score_ref[...] = jnp.zeros(score_ref.shape, jnp.float32)

    @pl.loop(0, layers)
    def _(l):
        lanes = pl.ds(pl.multiple_of(l * block, LANES), block)
        fill(l, lanes, 0)

        @pl.loop(0, queries // chunk)
        def _(n):
            at = pl.ds(pl.multiple_of(n * chunk, chunk), chunk)
            score_ref[:, at] += dot(lanes, scaled[0, at, :])


def prepare(queries, in_basis, out_basis, train):
    rows, features = queries.shape
    layers, width, _ = in_basis.shape
    cols = 2 * LANES
    wide = LANES // (cols // width) * width
    return pl.pallas_call(
        functools.partial(prepare_kernel, layers, width),
        in_specs=[HBM] * 4,
        out_specs=[VMEM] * 4,
        out_shape=[
            jax.ShapeDtypeStruct((rows, features), jnp.bfloat16),
            pltpu.VMEM((layers, cols, cols), jnp.bfloat16),
            pltpu.VMEM((layers, wide, wide), jnp.bfloat16),
            pltpu.VMEM(train.shape, train.dtype),
        ],
        scratch_shapes=[
            pltpu.VMEM(queries.shape, queries.dtype),
            pltpu.VMEM(in_basis.shape, in_basis.dtype),
            pltpu.VMEM(out_basis.shape, out_basis.dtype),
            pltpu.SemaphoreType.DMA((4,)),
        ],
        compiler_params=pltpu.CompilerParams(vmem_limit_bytes=16 * MIB),
        cost_estimate=pl.CostEstimate(
            flops=6 * 128 * features * 256, bytes_accessed=2 * train.size, transcendentals=0
        ),
        name="prepare",
    )(*[pltpu.with_memory_space_constraint(x, pltpu.HBM) for x in (queries, in_basis, out_basis, train)])


def rotate_train(train, first, second):
    rows, features = train.shape
    layers = first.shape[0]
    width = 1
    while layers * width * width < features:
        width *= 2
    return pl.pallas_call(
        functools.partial(train_kernel, layers, width),
        in_specs=[VMEM] * 3,
        out_specs=[VMEM] * 2,
        out_shape=[
            pltpu.VMEM((rows, features), jnp.bfloat16),
            jax.ShapeDtypeStruct((1, features), jnp.float32),
        ],
        compiler_params=pltpu.CompilerParams(vmem_limit_bytes=24 * MIB),
        cost_estimate=pl.CostEstimate(
            flops=6 * rows * features * 256, bytes_accessed=4 * rows * features, transcendentals=0
        ),
        name="rotate_train",
    )(train, first, second)


def choose_kernel(even_ref, odd_ref, out_ref):
    core = lax.axis_index("dp") % 2

    @pl.when(core == 0)
    def _():
        out_ref[...] = even_ref[...]

    @pl.when(core == 1)
    def _():
        out_ref[...] = odd_ref[...]


def choose(even, odd):
    return pl.pallas_call(
        choose_kernel,
        in_specs=[VMEM] * 2,
        out_specs=VMEM,
        out_shape=jax.ShapeDtypeStruct(even.shape, even.dtype),
        compiler_params=pltpu.CompilerParams(vmem_limit_bytes=4 * MIB),
        cost_estimate=pl.CostEstimate(
            flops=1000, bytes_accessed=4 * even.size, transcendentals=0
        ),
        name="choose",
    )(even, odd)


def score(steps, layer_group, damping, sums, rotated, pieces, train_rows):
    own, features = rotated.shape
    layers = layer_group.shape[0]
    rows = pieces[0].shape[0]
    count = len(pieces)
    queries = rows * count
    slots = layers if queries <= 512 else 1
    need = 12 * queries * features // layers * slots + 12 * own * queries
    return pl.pallas_call(
        functools.partial(score_kernel, layers, steps, rows, train_rows),
        in_specs=[SMEM, SMEM, VMEM, VMEM] + [VMEM] * count,
        out_specs=VMEM,
        out_shape=jax.ShapeDtypeStruct((own, queries), jnp.float32),
        scratch_shapes=[pltpu.VMEM((slots, queries, features // layers), jnp.float32)],
        compiler_params=pltpu.CompilerParams(vmem_limit_bytes=max(24 * MIB, need)),
        cost_estimate=pl.CostEstimate(
            flops=2 * own * queries * features, bytes_accessed=2 * own * features, transcendentals=0
        ),
        name="score",
    )(layer_group, damping, sums, pltpu.with_memory_space_constraint(rotated, pltpu.VMEM), *pieces)


def ring_order(chips):
    return list(range(0, chips, 2)) + list(range(chips - 1, 0, -2))


def per_device(train_grads, query_grads, in_basis, out_basis, damping, layer_group):
    devices = lax.axis_size("dp")
    chips = devices // 2
    order = ring_order(chips)
    pieces, steps = [], []

    def source(device, step):
        at = order.index(device // 2) - step
        return 2 * order[at % chips] + device % 2

    def ring(step, other=None):
        other = step if other is None else other
        return [(source(d, other if d % 2 else step), d) for d in range(devices)]

    def send(x, pairs):
        return lax.ppermute(x, "dp", pairs)

    def swap(x, bit):
        return send(x, [(i, i ^ bit) for i in range(devices)])

    def keep(chunk, step):
        pieces.extend([chunk, swap(chunk, 1)])
        steps.extend([(step, 0), (step, 1)])

    own, first, second, train = prepare(query_grads, in_basis, out_basis, train_grads)
    rotated, sums = rotate_train(train, first, second)
    far = chips // 2
    ahead = back = own
    keep(own, 0)
    for step in range(1, far):
        ahead = send(ahead, ring(1))
        keep(ahead, step)
        back = send(back, ring(-1))
        keep(back, -step)
    side = choose(ahead, back)
    keep(send(side, ring(1, -1)), far)
    if devices & (devices - 1):
        sums = lax.psum(sums, "dp")
    else:
        bit = 1
        while bit < devices:
            sums = sums + swap(sums, bit)
            bit *= 2

    return score(
        steps, layer_group, damping, sums, rotated, pieces, train_grads.shape[0] * devices
    )


def solution(mesh):
    placed = (P(("parts", "dp"), None), P(("parts", "dp"), None), P(), P(), P(), P())

    return jax.shard_map(
        per_device, mesh=mesh, in_specs=placed, out_specs=P(("parts", "dp"), None), check_vma=False
    )
```

```python
import functools

import jax
import jax.numpy as jnp
from jax import lax
from jax.experimental import pallas as pl
from jax.experimental.pallas import tpu as pltpu
from jax.sharding import PartitionSpec as P


LANES = 128
MIB = 1024 * 1024
VMEM = pl.BlockSpec(memory_space=pltpu.VMEM)
SMEM = pl.BlockSpec(memory_space=pltpu.SMEM)
HBM = pl.BlockSpec(memory_space=pltpu.HBM)


def stage_matrices(in_ref, out_ref, width):
    layers = in_ref.shape[0]
    group = 2 * LANES // width
    half = LANES // group
    cols, wide = 2 * LANES, half * width

    def iota(shape, dim):
        return lax.broadcasted_iota(jnp.int32, shape, dim)

    spread = iota((width, cols), 1) // group == iota((width, cols), 0)
    repeat = iota((width, wide), 1) % width == iota((width, wide), 0)
    flat_in = in_ref[...].reshape(layers * width, width)
    flat_out = out_ref[...].reshape(layers * width, width)
    wide_in = jnp.dot(flat_in, spread.astype(jnp.bfloat16), preferred_element_type=jnp.float32)
    wide_out = jnp.dot(flat_out, repeat.astype(jnp.bfloat16), preferred_element_type=jnp.float32)
    which = iota((width, cols), 1) % group
    keep = iota((LANES, wide), 0) // group == iota((LANES, wide), 1) // width
    firsts, seconds = [], []
    for l in range(layers):
        rows = wide_in[l * width : (l + 1) * width]
        first = [jnp.where(which == i, rows, 0.0) for i in range(group)]
        firsts.append(jnp.concatenate(first, axis=0).astype(jnp.bfloat16))
        second = []
        for k in range(width // group):
            at = l * width + k * group
            tiled = jnp.concatenate([wide_out[at : at + group]] * half, axis=0)
            second.append(jnp.where(keep, tiled, 0.0))
        seconds.append(jnp.concatenate(second, axis=0).astype(jnp.bfloat16))
    return firsts, seconds


def rotate_layer(x_ref, base, first, second, width):
    cols = 2 * LANES
    inner = []
    for k in range(width * width // cols):
        at = base + k * cols
        inner.append(
            jnp.dot(x_ref[:, at : at + cols], first, preferred_element_type=jnp.float32).astype(
                jnp.bfloat16
            )
        )
    for h in range(2):
        lhs = jnp.concatenate([x[:, h * LANES : (h + 1) * LANES] for x in inner], axis=1)
        yield jnp.dot(lhs, second, preferred_element_type=jnp.float32)


def prepare_kernel(
    layers,
    width,
    q_hbm,
    in_hbm,
    out_hbm,
    x_hbm,
    rot_ref,
    first_ref,
    second_ref,
    held_ref,
    q_ref,
    in_ref,
    out_ref,
    sems,
):
    held = x_hbm.at[:, pl.ds(0, held_ref.shape[1])]
    ends = ((in_hbm, in_ref), (out_hbm, out_ref), (q_hbm, q_ref), (held, held_ref))
    copies = [pltpu.make_async_copy(a, b, sems.at[i]) for i, (a, b) in enumerate(ends)]
    for copy in copies:
        copy.start()
    for copy in copies[:3]:
        copy.wait()
    firsts, seconds = stage_matrices(in_ref, out_ref, width)
    rows = q_ref.shape[0]
    cols, block = 2 * LANES, width * width
    tiles = block // cols
    inners = []
    for l in range(layers):
        stack = [
            q_ref[:, l * block + k * cols : l * block + (k + 1) * cols].astype(jnp.float32)
            for k in range(tiles)
        ]
        stack = jnp.concatenate(stack, axis=0).astype(jnp.bfloat16)
        inners.append(jnp.dot(stack, firsts[l], preferred_element_type=jnp.float32))
    for l in range(layers):
        halves = [
            jnp.concatenate(
                [
                    inners[l][k * rows : (k + 1) * rows, h * LANES : (h + 1) * LANES]
                    for k in range(tiles)
                ],
                axis=1,
            )
            for h in range(2)
        ]
        lhs = jnp.concatenate(halves, axis=0).astype(jnp.bfloat16)
        rotated = jnp.dot(lhs, seconds[l], preferred_element_type=jnp.float32).astype(jnp.bfloat16)
        at = l * block
        for h in range(2):
            rot_ref[:, at : at + block // 2] = rotated[h * rows : (h + 1) * rows]
            at += block // 2
    for l in range(layers):
        first_ref[l] = firsts[l]
        second_ref[l] = seconds[l]
    copies[3].wait()


def train_kernel(
    layers,
    width,
    early,
    x_hbm,
    held_ref,
    first_ref,
    second_ref,
    rot_ref,
    sums_ref,
    late_ref,
    sems,
):
    block = width * width
    copies = []
    for l in range(early, layers):
        source = x_hbm.at[:, pl.ds(l * block, block)]
        copies.append(pltpu.make_async_copy(source, late_ref.at[l - early], sems.at[l - early]))
        copies[-1].start()
    for l in range(layers):
        at = l * block
        if l >= early:
            copies[l - early].wait()
        x_ref, base = (held_ref, at) if l < early else (late_ref.at[l - early], 0)
        for rotated in rotate_layer(x_ref, base, first_ref[l], second_ref[l], width):
            rot_ref[:, at : at + block // 2] = rotated.astype(jnp.bfloat16)
            sums_ref[:, at : at + block // 2] = jnp.sum(rotated * rotated, axis=0, keepdims=True)
            at += block // 2


def score_kernel(
    layers, steps, rows, train_rows, group_ref, damping_ref, sums_ref, rot_ref, *refs
):
    count = len(steps)
    chips = lax.axis_size("dp") // 2
    me = lax.axis_index("dp")
    chip, mine = me // 2, me % 2
    spot = jnp.where(chip % 2 == 0, chip // 2, chips - 1 - chip // 2)
    pieces, score_ref, scaled = refs[:count], refs[count], refs[count + 1 :]
    block = sums_ref.shape[1] // layers
    spots = []
    for step, twin in steps:
        at = (spot - step + chips) % chips
        first = jnp.where(at < chips // 2, 2 * at, 2 * (chips - 1 - at) + 1) * 2
        spots.append(pl.multiple_of((first + (mine ^ twin)) * rows, 8))

    def fill(l, lanes, slot):
        numbers = lax.broadcasted_iota(jnp.int32, group_ref.shape, 1)
        group = jnp.sum(jnp.where(numbers == l, group_ref[...], 0), axis=1, keepdims=True)
        damps = lax.broadcasted_iota(jnp.int32, damping_ref.shape, 1) == group
        damp = jnp.sum(jnp.where(damps, damping_ref[...], 0.0), axis=1, keepdims=True)
        corrected = sums_ref[:, lanes] / train_rows
        mean = jnp.mean(corrected, axis=1, keepdims=True)
        inverse = 1.0 / (corrected + damp * mean)
        for where, piece in zip(spots, pieces):
            scaled[slot][pl.ds(where, rows), :] = piece[:, lanes].astype(jnp.float32) * inverse

    def dot(lanes, right):
        return lax.dot_general(
            rot_ref[:, lanes],
            right.astype(jnp.bfloat16),
            (((1,), (1,)), ((), ())),
            preferred_element_type=jnp.float32,
        )

    if len(scaled) == layers:
        total = None
        for l in range(layers):
            fill(l, slice(l * block, (l + 1) * block), l)
        for l in range(layers):
            product = dot(slice(l * block, (l + 1) * block), scaled[l][...])
            total = product if total is None else total + product
        score_ref[...] = total
        return

    queries = score_ref.shape[1]
    chunk = next(n for n in (512, 384, 256, 128, queries) if queries % n == 0)
    score_ref[...] = jnp.zeros(score_ref.shape, jnp.float32)

    @pl.loop(0, layers)
    def _(l):
        lanes = pl.ds(pl.multiple_of(l * block, LANES), block)
        fill(l, lanes, 0)

        @pl.loop(0, queries // chunk)
        def _(n):
            at = pl.ds(pl.multiple_of(n * chunk, chunk), chunk)
            score_ref[:, at] += dot(lanes, scaled[0][at, :])


def prepare(queries, in_basis, out_basis, train, early):
    rows, features = queries.shape
    layers, width, _ = in_basis.shape
    cols = 2 * LANES
    wide = LANES // (cols // width) * width
    return pl.pallas_call(
        functools.partial(prepare_kernel, layers, width),
        in_specs=[HBM] * 4,
        out_specs=[VMEM] * 4,
        out_shape=[
            jax.ShapeDtypeStruct((rows, features), jnp.bfloat16),
            pltpu.VMEM((layers, cols, cols), jnp.bfloat16),
            pltpu.VMEM((layers, wide, wide), jnp.bfloat16),
            pltpu.VMEM((train.shape[0], features // layers * early), train.dtype),
        ],
        scratch_shapes=[
            pltpu.VMEM(queries.shape, queries.dtype),
            pltpu.VMEM(in_basis.shape, in_basis.dtype),
            pltpu.VMEM(out_basis.shape, out_basis.dtype),
            pltpu.SemaphoreType.DMA((4,)),
        ],
        compiler_params=pltpu.CompilerParams(vmem_limit_bytes=16 * MIB),
        cost_estimate=pl.CostEstimate(
            flops=6 * 128 * features * 256, bytes_accessed=2 * train.size, transcendentals=0
        ),
        name="prepare",
    )(*[pltpu.with_memory_space_constraint(x, pltpu.HBM) for x in (queries, in_basis, out_basis, train)])


def rotate_train(train, held, first, second, width):
    rows, features = train.shape
    layers = first.shape[0]
    block = features // layers
    early = held.shape[1] // block
    late = layers - early
    return pl.pallas_call(
        functools.partial(train_kernel, layers, width, early),
        in_specs=[HBM] + [VMEM] * 3,
        out_specs=[VMEM] * 2,
        out_shape=[
            pltpu.VMEM((rows, features), jnp.bfloat16),
            jax.ShapeDtypeStruct((1, features), jnp.float32),
        ],
        scratch_shapes=[
            pltpu.VMEM((max(late, 1), rows, block), train.dtype),
            pltpu.SemaphoreType.DMA((max(late, 1),)),
        ],
        compiler_params=pltpu.CompilerParams(vmem_limit_bytes=24 * MIB),
        cost_estimate=pl.CostEstimate(
            flops=6 * rows * features * 256, bytes_accessed=4 * rows * features, transcendentals=0
        ),
        name="rotate_train",
    )(pltpu.with_memory_space_constraint(train, pltpu.HBM), held, first, second)


def choose_kernel(even_ref, odd_ref, out_ref):
    core = lax.axis_index("dp") % 2

    @pl.when(core == 0)
    def _():
        out_ref[...] = even_ref[...]

    @pl.when(core == 1)
    def _():
        out_ref[...] = odd_ref[...]


def choose(even, odd):
    return pl.pallas_call(
        choose_kernel,
        in_specs=[VMEM] * 2,
        out_specs=VMEM,
        out_shape=jax.ShapeDtypeStruct(even.shape, even.dtype),
        compiler_params=pltpu.CompilerParams(vmem_limit_bytes=4 * MIB),
        cost_estimate=pl.CostEstimate(
            flops=1000, bytes_accessed=4 * even.size, transcendentals=0
        ),
        name="choose",
    )(even, odd)


def score(steps, layer_group, damping, sums, rotated, pieces, train_rows):
    own, features = rotated.shape
    layers = layer_group.shape[0]
    rows = pieces[0].shape[0]
    count = len(pieces)
    queries = rows * count
    slots = layers if queries <= 512 else 1
    need = 12 * queries * features // layers * slots + 12 * own * queries
    return pl.pallas_call(
        functools.partial(score_kernel, layers, steps, rows, train_rows),
        in_specs=[VMEM] * (4 + count),
        out_specs=VMEM,
        out_shape=jax.ShapeDtypeStruct((own, queries), jnp.float32),
        scratch_shapes=[pltpu.VMEM((queries, features // layers), jnp.float32)] * slots,
        compiler_params=pltpu.CompilerParams(vmem_limit_bytes=max(24 * MIB, need)),
        cost_estimate=pl.CostEstimate(
            flops=2 * own * queries * features, bytes_accessed=2 * own * features, transcendentals=0
        ),
        name="score",
    )(layer_group[None], damping[None], sums, pltpu.with_memory_space_constraint(rotated, pltpu.VMEM), *pieces)


def ring_order(chips):
    return list(range(0, chips, 2)) + list(range(chips - 1, 0, -2))


def per_device(train_grads, query_grads, in_basis, out_basis, damping, layer_group):
    devices = lax.axis_size("dp")
    chips = devices // 2
    order = ring_order(chips)
    pieces, steps = [], []

    def source(device, step):
        at = order.index(device // 2) - step
        return 2 * order[at % chips] + device % 2

    def ring(step, other=None):
        other = step if other is None else other
        return [(source(d, other if d % 2 else step), d) for d in range(devices)]

    def send(x, pairs):
        return lax.ppermute(x, "dp", pairs)

    def swap(x, bit):
        return send(x, [(i, i ^ bit) for i in range(devices)])

    def keep(chunk, step):
        pieces.extend([chunk, swap(chunk, 1)])
        steps.extend([(step, 0), (step, 1)])

    layers, width, _ = in_basis.shape
    early = (layers + 1) // 2
    own, first, second, held = prepare(query_grads, in_basis, out_basis, train_grads, early)
    rotated, sums = rotate_train(train_grads, held, first, second, width)
    far = chips // 2
    ahead = back = own
    keep(own, 0)
    for step in range(1, far):
        ahead = send(ahead, ring(1))
        keep(ahead, step)
        back = send(back, ring(-1))
        keep(back, -step)
    side = choose(ahead, back)
    keep(send(side, ring(1, -1)), far)
    if devices & (devices - 1):
        sums = lax.psum(sums, "dp")
    else:
        bit = 1
        while bit < devices:
            sums = sums + swap(sums, bit)
            bit *= 2

    return score(
        steps, layer_group, damping, sums, rotated, pieces, train_grads.shape[0] * devices
    )


def solution(mesh):
    placed = (P(("parts", "dp"), None), P(("parts", "dp"), None), P(), P(), P(), P())

    return jax.shard_map(
        per_device, mesh=mesh, in_specs=placed, out_specs=P(("parts", "dp"), None), check_vma=False
    )
```

```python
import functools

import jax
import jax.numpy as jnp
from jax import lax
from jax.experimental import pallas as pl
from jax.experimental.pallas import tpu as pltpu
from jax.sharding import PartitionSpec as P


LANES = 128
MIB = 1024 * 1024
VMEM = pl.BlockSpec(memory_space=pltpu.VMEM)
SMEM = pl.BlockSpec(memory_space=pltpu.SMEM)
HBM = pl.BlockSpec(memory_space=pltpu.HBM)


def stage_matrices(in_ref, out_ref, width):
    layers = in_ref.shape[0]
    group = 2 * LANES // width
    half = LANES // group
    cols, wide = 2 * LANES, half * width

    def iota(shape, dim):
        return lax.broadcasted_iota(jnp.int32, shape, dim)

    spread = iota((width, cols), 1) // group == iota((width, cols), 0)
    repeat = iota((width, wide), 1) % width == iota((width, wide), 0)
    flat_in = in_ref[...].reshape(layers * width, width)
    flat_out = out_ref[...].reshape(layers * width, width)
    wide_in = jnp.dot(flat_in, spread.astype(jnp.bfloat16), preferred_element_type=jnp.float32)
    wide_out = jnp.dot(flat_out, repeat.astype(jnp.bfloat16), preferred_element_type=jnp.float32)
    which = iota((width, cols), 1) % group
    keep = iota((LANES, wide), 0) // group == iota((LANES, wide), 1) // width
    firsts, seconds = [], []
    for l in range(layers):
        rows = wide_in[l * width : (l + 1) * width]
        first = [jnp.where(which == i, rows, 0.0) for i in range(group)]
        firsts.append(jnp.concatenate(first, axis=0).astype(jnp.bfloat16))
        second = []
        for k in range(width // group):
            at = l * width + k * group
            tiled = jnp.concatenate([wide_out[at : at + group]] * half, axis=0)
            second.append(jnp.where(keep, tiled, 0.0))
        seconds.append(jnp.concatenate(second, axis=0).astype(jnp.bfloat16))
    return firsts, seconds


def rotate_layer(x_ref, base, first, second, width):
    cols = 2 * LANES
    inner = []
    for k in range(width * width // cols):
        at = base + k * cols
        inner.append(
            jnp.dot(x_ref[:, at : at + cols], first, preferred_element_type=jnp.float32).astype(
                jnp.bfloat16
            )
        )
    for h in range(2):
        lhs = jnp.concatenate([x[:, h * LANES : (h + 1) * LANES] for x in inner], axis=1)
        yield jnp.dot(lhs, second, preferred_element_type=jnp.float32)


def prepare_kernel(
    layers,
    width,
    q_hbm,
    in_hbm,
    out_hbm,
    x_hbm,
    rot_ref,
    first_ref,
    second_ref,
    held_ref,
    q_ref,
    in_ref,
    out_ref,
    sems,
):
    held = x_hbm.at[:, pl.ds(0, held_ref.shape[1])]
    ends = ((in_hbm, in_ref), (out_hbm, out_ref), (q_hbm, q_ref), (held, held_ref))
    copies = [pltpu.make_async_copy(a, b, sems.at[i]) for i, (a, b) in enumerate(ends)]
    for copy in copies:
        copy.start()
    for copy in copies[:3]:
        copy.wait()
    firsts, seconds = stage_matrices(in_ref, out_ref, width)
    rows = q_ref.shape[0]
    cols, block = 2 * LANES, width * width
    tiles = block // cols
    inners = []
    for l in range(layers):
        stack = [
            q_ref[:, l * block + k * cols : l * block + (k + 1) * cols].astype(jnp.float32)
            for k in range(tiles)
        ]
        stack = jnp.concatenate(stack, axis=0).astype(jnp.bfloat16)
        inners.append(jnp.dot(stack, firsts[l], preferred_element_type=jnp.float32))
    for l in range(layers):
        halves = [
            jnp.concatenate(
                [
                    inners[l][k * rows : (k + 1) * rows, h * LANES : (h + 1) * LANES]
                    for k in range(tiles)
                ],
                axis=1,
            )
            for h in range(2)
        ]
        lhs = jnp.concatenate(halves, axis=0).astype(jnp.bfloat16)
        rotated = jnp.dot(lhs, seconds[l], preferred_element_type=jnp.float32).astype(jnp.bfloat16)
        at = l * block
        for h in range(2):
            rot_ref[:, at : at + block // 2] = rotated[h * rows : (h + 1) * rows]
            at += block // 2
    for l in range(layers):
        first_ref[l] = firsts[l]
        second_ref[l] = seconds[l]
    copies[3].wait()


def train_kernel(
    layers,
    width,
    early,
    x_hbm,
    held_ref,
    first_ref,
    second_ref,
    rot_ref,
    sums_ref,
    late_ref,
    sems,
):
    block = width * width
    copies = []
    for l in range(early, layers):
        source = x_hbm.at[:, pl.ds(l * block, block)]
        copies.append(pltpu.make_async_copy(source, late_ref.at[l - early], sems.at[l - early]))
        copies[-1].start()
    for l in range(layers):
        at = l * block
        if l >= early:
            copies[l - early].wait()
        x_ref, base = (held_ref, at) if l < early else (late_ref.at[l - early], 0)
        for rotated in rotate_layer(x_ref, base, first_ref[l], second_ref[l], width):
            rot_ref[:, at : at + block // 2] = rotated.astype(jnp.bfloat16)
            sums_ref[:, at : at + block // 2] = jnp.sum(rotated * rotated, axis=0, keepdims=True)
            at += block // 2


def score_kernel(
    layers, steps, rows, train_rows, group_ref, damping_ref, sums_ref, rot_ref, *refs
):
    count = len(steps)
    chips = lax.axis_size("dp") // 2
    me = lax.axis_index("dp")
    chip, mine = me // 2, me % 2
    spot = jnp.where(chip % 2 == 0, chip // 2, chips - 1 - chip // 2)
    pieces, score_ref, scaled = refs[:count], refs[count], refs[count + 1 : -2]
    held, sems = refs[-2:]
    block = sums_ref.shape[1] // layers
    spots = []
    for step, twin in steps:
        at = (spot - step + chips) % chips
        first = jnp.where(at < chips // 2, 2 * at, 2 * (chips - 1 - at) + 1) * 2
        spots.append(pl.multiple_of((first + (mine ^ twin)) * rows, 8))

    def fill(l, lanes, slot):
        numbers = lax.broadcasted_iota(jnp.int32, group_ref.shape, 1)
        group = jnp.sum(jnp.where(numbers == l, group_ref[...], 0), axis=1, keepdims=True)
        damps = lax.broadcasted_iota(jnp.int32, damping_ref.shape, 1) == group
        damp = jnp.sum(jnp.where(damps, damping_ref[...], 0.0), axis=1, keepdims=True)
        corrected = sums_ref[:, lanes] / train_rows
        mean = jnp.mean(corrected, axis=1, keepdims=True)
        inverse = 1.0 / (corrected + damp * mean)
        for where, piece in zip(spots, pieces):
            scaled[slot][pl.ds(where, rows), :] = piece[:, lanes].astype(jnp.float32) * inverse

    def dot(lanes, right, part=slice(None)):
        return lax.dot_general(
            rot_ref[part, lanes],
            right.astype(jnp.bfloat16),
            (((1,), (1,)), ((), ())),
            preferred_element_type=jnp.float32,
        )

    if len(scaled) == layers:
        for l in range(layers):
            fill(l, slice(l * block, (l + 1) * block), l)
        own = rot_ref.shape[0]
        size = own // 2 if own % 32 == 0 else own
        copies = []
        for at in range(0, own, size):
            total = None
            for l in range(layers):
                lanes = slice(l * block, (l + 1) * block)
                product = dot(lanes, scaled[l][...], slice(at, at + size))
                total = product if total is None else total + product
            held[at : at + size, :] = total
            part = pl.ds(at, size)
            copies.append(
                pltpu.make_async_copy(held.at[part], score_ref.at[part], sems.at[len(copies)])
            )
            copies[-1].start()
        for copy in copies:
            copy.wait()
        return

    queries = score_ref.shape[1]
    chunk = next(n for n in (512, 384, 256, 128, queries) if queries % n == 0)
    held[...] = jnp.zeros(held.shape, jnp.float32)

    @pl.loop(0, layers)
    def _(l):
        lanes = pl.ds(pl.multiple_of(l * block, LANES), block)
        fill(l, lanes, 0)

        @pl.loop(0, queries // chunk)
        def _(n):
            at = pl.ds(pl.multiple_of(n * chunk, chunk), chunk)
            held[:, at] += dot(lanes, scaled[0][at, :])

    copy = pltpu.make_async_copy(held, score_ref, sems.at[0])
    copy.start()
    copy.wait()


def prepare(queries, in_basis, out_basis, train, early):
    rows, features = queries.shape
    layers, width, _ = in_basis.shape
    cols = 2 * LANES
    wide = LANES // (cols // width) * width
    return pl.pallas_call(
        functools.partial(prepare_kernel, layers, width),
        in_specs=[HBM] * 4,
        out_specs=[VMEM] * 4,
        out_shape=[
            jax.ShapeDtypeStruct((rows, features), jnp.bfloat16),
            pltpu.VMEM((layers, cols, cols), jnp.bfloat16),
            pltpu.VMEM((layers, wide, wide), jnp.bfloat16),
            pltpu.VMEM((train.shape[0], features // layers * early), train.dtype),
        ],
        scratch_shapes=[
            pltpu.VMEM(queries.shape, queries.dtype),
            pltpu.VMEM(in_basis.shape, in_basis.dtype),
            pltpu.VMEM(out_basis.shape, out_basis.dtype),
            pltpu.SemaphoreType.DMA((4,)),
        ],
        compiler_params=pltpu.CompilerParams(vmem_limit_bytes=16 * MIB),
        cost_estimate=pl.CostEstimate(
            flops=6 * 128 * features * 256, bytes_accessed=2 * train.size, transcendentals=0
        ),
        name="prepare",
    )(*[pltpu.with_memory_space_constraint(x, pltpu.HBM) for x in (queries, in_basis, out_basis, train)])


def rotate_train(train, held, first, second, width):
    rows, features = train.shape
    layers = first.shape[0]
    block = features // layers
    early = held.shape[1] // block
    late = layers - early
    return pl.pallas_call(
        functools.partial(train_kernel, layers, width, early),
        in_specs=[HBM] + [VMEM] * 3,
        out_specs=[VMEM] * 2,
        out_shape=[
            pltpu.VMEM((rows, features), jnp.bfloat16),
            jax.ShapeDtypeStruct((1, features), jnp.float32),
        ],
        scratch_shapes=[
            pltpu.VMEM((max(late, 1), rows, block), train.dtype),
            pltpu.SemaphoreType.DMA((max(late, 1),)),
        ],
        compiler_params=pltpu.CompilerParams(vmem_limit_bytes=24 * MIB),
        cost_estimate=pl.CostEstimate(
            flops=6 * rows * features * 256, bytes_accessed=4 * rows * features, transcendentals=0
        ),
        name="rotate_train",
    )(pltpu.with_memory_space_constraint(train, pltpu.HBM), held, first, second)


def choose_kernel(even_ref, odd_ref, out_ref):
    core = lax.axis_index("dp") % 2

    @pl.when(core == 0)
    def _():
        out_ref[...] = even_ref[...]

    @pl.when(core == 1)
    def _():
        out_ref[...] = odd_ref[...]


def choose(even, odd):
    return pl.pallas_call(
        choose_kernel,
        in_specs=[VMEM] * 2,
        out_specs=VMEM,
        out_shape=jax.ShapeDtypeStruct(even.shape, even.dtype),
        compiler_params=pltpu.CompilerParams(vmem_limit_bytes=4 * MIB),
        cost_estimate=pl.CostEstimate(
            flops=1000, bytes_accessed=4 * even.size, transcendentals=0
        ),
        name="choose",
    )(even, odd)


def score(steps, layer_group, damping, sums, rotated, pieces, train_rows):
    own, features = rotated.shape
    layers = layer_group.shape[0]
    rows = pieces[0].shape[0]
    count = len(pieces)
    queries = rows * count
    slots = layers if queries <= 512 else 1
    need = 12 * queries * features // layers * slots + 12 * own * queries
    return pl.pallas_call(
        functools.partial(score_kernel, layers, steps, rows, train_rows),
        in_specs=[VMEM] * (4 + count),
        out_specs=HBM,
        out_shape=jax.ShapeDtypeStruct((own, queries), jnp.float32),
        scratch_shapes=[pltpu.VMEM((queries, features // layers), jnp.float32)] * slots
        + [pltpu.VMEM((own, queries), jnp.float32), pltpu.SemaphoreType.DMA((2,))],
        compiler_params=pltpu.CompilerParams(vmem_limit_bytes=max(24 * MIB, need)),
        cost_estimate=pl.CostEstimate(
            flops=2 * own * queries * features, bytes_accessed=2 * own * features, transcendentals=0
        ),
        name="score",
    )(layer_group[None], damping[None], sums, pltpu.with_memory_space_constraint(rotated, pltpu.VMEM), *pieces)


def ring_order(chips):
    return list(range(0, chips, 2)) + list(range(chips - 1, 0, -2))


def per_device(train_grads, query_grads, in_basis, out_basis, damping, layer_group):
    devices = lax.axis_size("dp")
    chips = devices // 2
    order = ring_order(chips)
    pieces, steps = [], []

    def source(device, step):
        at = order.index(device // 2) - step
        return 2 * order[at % chips] + device % 2

    def ring(step, other=None):
        other = step if other is None else other
        return [(source(d, other if d % 2 else step), d) for d in range(devices)]

    def send(x, pairs):
        return lax.ppermute(x, "dp", pairs)

    def swap(x, bit):
        return send(x, [(i, i ^ bit) for i in range(devices)])

    def keep(chunk, step):
        pieces.extend([chunk, swap(chunk, 1)])
        steps.extend([(step, 0), (step, 1)])

    layers, width, _ = in_basis.shape
    early = (layers + 1) // 2
    own, first, second, held = prepare(query_grads, in_basis, out_basis, train_grads, early)
    rotated, sums = rotate_train(train_grads, held, first, second, width)
    far = chips // 2
    ahead = back = own
    keep(own, 0)
    for step in range(1, far):
        ahead = send(ahead, ring(1))
        keep(ahead, step)
        back = send(back, ring(-1))
        keep(back, -step)
    side = choose(ahead, back)
    keep(send(side, ring(1, -1)), far)
    if devices & (devices - 1):
        sums = lax.psum(sums, "dp")
    else:
        bit = 1
        while bit < devices:
            sums = sums + swap(sums, bit)
            bit *= 2

    return score(
        steps, layer_group, damping, sums, rotated, pieces, train_grads.shape[0] * devices
    )


def solution(mesh):
    placed = (P(("parts", "dp"), None), P(("parts", "dp"), None), P(), P(), P(), P())

    return jax.shard_map(
        per_device, mesh=mesh, in_specs=placed, out_specs=P(("parts", "dp"), None), check_vma=False
    )
```
